32 devices in a mesh: groups: 2 (over x), expert: 16 (over z, y, core).
Axes of the slice: x: 2, y: 2, z: 4, core: 2. Of those that a mesh axis runs over, the one named last changes fastest.
Arguments:
- query_features: bfloat16 [4096, 1024], P(('groups', 'expert')), parts along dimension 0, may hold values from -6 to 6
- query_job_label: int32 [4096], P(('groups', 'expert')), parts along dimension 0, may hold values from 0 to 7, as said below
- selected_specialists: int32 [4096, 2], P(('groups', 'expert')), parts along dimension 0, may hold values from 0 to 8, as said below
- whole_number_mixing_factors: int32 [4096, 2], P(('groups', 'expert')), parts along dimension 0, may hold values from 1 to 8
- copy_room_sizes: int32 [16], replicated, may hold values from 256 to 384, as said below
- first_layer_matrix: bfloat16 [16, 1024, 2048], P('expert'), as said below
- second_layer_matrix: bfloat16 [16, 2048, 1024], P('expert'), as said below
Outputs:
- mixture: bfloat16 [4096, 1024], P(('groups', 'expert')), parts along dimension 0
The draws below stay inside these ranges and needn't reach their ends.
There are 2 independent parts, one for each index of `groups`. The reference program is written for one: setup_inputs(seed, part) draws one part's arguments, and reference() takes and returns one part's arrays. A program takes and returns all parts, laid end to end along the dimension named above; an argument that names none is the same for every part. Nothing has to cross between parts.
Inputs may be any that keep to these rules, and one draw needn't show every extreme that they name: `query_job_label`: each request's task number; column 0 of `selected_specialists` names a task expert of this task. `selected_specialists`: column 0 names a task expert of the row's task (number r from 8 on is task expert r - 8), column 1 a shared expert (below 8). From the rows of one device at most 32 entries go to one expert copy, and in every draw some copy receives exactly 32 entries from every device. `copy_room_sizes`: some copy has capacity 384 and some copy 2 * 128. `first_layer_matrix`: the 1 copies of one shared expert hold equal weights. `second_layer_matrix`: the 1 copies of one shared expert hold equal weights.
All inputs are finite; a program needn't handle non-finite values.
Results may differ from the reference program's by a relative error of at most 0.0058.
Values may be sent and summed in bfloat16 or wider, within the bound.
A program may use at most 64 MiB of HBM per device.

```python
import jax
import jax.numpy as jnp
from jax import lax

D = 1024
HIDDEN_SIZE = 2048
TASKS = 8
SHARED = 8
TOP = 2
ROWS_DEV = 128
EXPERTS = 16
REPL = 1
TASK_EXP = 1
SLOT = 32
CAPACITY = 384
ROWS = 2048


def pick_tickets(device_key, popular, hottest, wanted, slots):
    tickets = popular.shape[0] * slots
    owners = jnp.arange(tickets, dtype=jnp.int32) // slots
    jitter = jax.random.randint(jax.random.fold_in(device_key, 1), (tickets,), 0, 16384)
    scores = jitter + popular[owners] + jnp.where(owners == hottest, 1 << 20, 0)
    ranking = jnp.argsort(-scores, stable=True)
    chosen = owners[ranking[:wanted]]
    shuffled = jax.random.permutation(jax.random.fold_in(device_key, 2), wanted)
    return chosen[shuffled]


def routing_plan(key):
    base_key = jax.random.fold_in(key, 11)
    task_copies = TASKS * TASK_EXP
    group_rows = ROWS_DEV // REPL
    task_popular = jax.random.randint(jax.random.fold_in(base_key, 1), (task_copies,), 0, 8192)
    task_hottest = jax.random.randint(jax.random.fold_in(base_key, 2), (), 0, task_copies)
    shared_popular = jax.random.randint(jax.random.fold_in(base_key, 3), (SHARED,), 0, 8192)
    shared_hottest = jax.random.randint(jax.random.fold_in(base_key, 4), (), 0, SHARED)
    task_base = jax.random.fold_in(base_key, 5)
    shared_base = jax.random.fold_in(base_key, 6)

    def task_device(device):
        return pick_tickets(jax.random.fold_in(task_base, device), task_popular, task_hottest, ROWS_DEV, SLOT)

    def shared_group(group):
        return pick_tickets(jax.random.fold_in(shared_base, group), shared_popular, shared_hottest, group_rows, SLOT)
    task_choice = jax.vmap(task_device)(jnp.arange(EXPERTS, dtype=jnp.int32)).reshape(ROWS)
    shared_choice = jax.vmap(shared_group)(jnp.arange(EXPERTS * REPL, dtype=jnp.int32))
    shared_flat = shared_choice.reshape(EXPERTS, REPL, group_rows).transpose(0, 2, 1).reshape(ROWS)
    tasks = (task_choice // TASK_EXP).astype(jnp.int32)
    numbers = SHARED + task_choice % TASK_EXP
    routing = jnp.stack([numbers, shared_flat], axis=1).astype(jnp.int32)
    return (tasks, routing)


def draw_query_job_label(key, part):
    return routing_plan(key)[0]


def draw_selected_specialists(key, part):
    return routing_plan(key)[1]


def draw_copy_room_sizes(key, part):
    values = jax.random.randint(jax.random.fold_in(key, 1), (EXPERTS,), 2 * ROWS_DEV, CAPACITY + 1)
    top_at = jax.random.randint(jax.random.fold_in(key, 2), (), 0, EXPERTS)
    low_at = (top_at + jax.random.randint(jax.random.fold_in(key, 3), (), 1, EXPERTS)) % EXPERTS
    indices = jnp.arange(EXPERTS, dtype=jnp.int32)
    values = jnp.where(indices == top_at, CAPACITY, values)
    values = jnp.where(indices == low_at, 2 * ROWS_DEV, values)
    return values.astype(jnp.int32)


def copied_weights(key, rows_in, cols_out):
    task_copies = TASKS * TASK_EXP
    shared_part = jax.random.normal(jax.random.fold_in(key, 1), (SHARED, rows_in, cols_out), jnp.float32)
    task_part = jax.random.normal(jax.random.fold_in(key, 2), (task_copies, rows_in, cols_out), jnp.float32)
    stacked = jnp.concatenate([jnp.repeat(shared_part, REPL, axis=0), task_part], axis=0)
    return (stacked * rows_in ** (-0.5)).astype(jnp.bfloat16)


def draw_first_layer_matrix(key, part):
    return copied_weights(jax.random.fold_in(key, 21), D, HIDDEN_SIZE)


def draw_second_layer_matrix(key, part):
    return copied_weights(jax.random.fold_in(key, 22), HIDDEN_SIZE, D)


def place_ends(array, key, least, top_value):
    longest = array.shape.index(max(array.shape))
    spots = []
    for shift in (0, 1):
        where = [jax.random.randint(jax.random.fold_in(key, axis), (), 0, length) for axis, length in enumerate(array.shape)]
        where[longest] = (where[longest] + shift) % array.shape[longest]
        spots.append(tuple(where))
    return array.at[spots[0]].set(least).at[spots[1]].set(top_value)


def block_scale(stream_key, extent, split, smallest, largest):
    def one(position, shards_of):
        draws = jax.random.uniform(jax.random.fold_in(jax.random.fold_in(stream_key, 6), position), (shards_of,), jnp.float32, smallest / len(split), largest / len(split))
        return jnp.repeat(jnp.exp(draws), extent[position] // shards_of).reshape((-1,) + (1,) * (len(extent) - position - 1))

    loudness = one(*split[0])
    for cut in split[1:]:
        loudness = loudness * one(*cut)
    return loudness


def noise(stream_key, shape, deviation, limit, split=(), kind=jnp.bfloat16):
    array = deviation * jax.random.normal(stream_key, shape, jnp.float32)
    if split:
        array = array * block_scale(stream_key, shape, split, -0.22, 0.18)
    return jnp.clip(array, -limit, limit).astype(kind)


def setup_inputs(seed: int = 0, part: int = 0) -> dict:
    splits = jax.random.split(jax.random.key(seed), 8)
    part_splits = jax.random.split(jax.random.fold_in(splits[7], part), 8)
    return {
        "query_features": noise(part_splits[0], (ROWS, D), 1.0, 6.0, ((0, 16),)),
        "query_job_label": draw_query_job_label(jax.random.fold_in(jax.random.fold_in(splits[7], part), 71), part),
        "selected_specialists": draw_selected_specialists(jax.random.fold_in(jax.random.fold_in(splits[7], part), 71), part),
        "whole_number_mixing_factors": place_ends(jax.random.randint(part_splits[3], (ROWS, TOP), 1, 9), jax.random.fold_in(part_splits[3], 1), 1, 8).astype(jnp.int32),
        "copy_room_sizes": draw_copy_room_sizes(jax.random.fold_in(splits[7], 71), part),
        "first_layer_matrix": draw_first_layer_matrix(jax.random.fold_in(splits[7], 71), part),
        "second_layer_matrix": draw_second_layer_matrix(jax.random.fold_in(splits[7], 71), part),
    }


def expert_mlp(block_rows, up_matrix, down_matrix):
    hidden = jax.nn.gelu(jnp.dot(block_rows, up_matrix, preferred_element_type=jnp.float32)).astype(jnp.bfloat16)
    return jnp.dot(hidden, down_matrix, preferred_element_type=jnp.float32).astype(jnp.bfloat16)


def reference(query_features, query_job_label, selected_specialists, whole_number_mixing_factors, copy_room_sizes, first_layer_matrix, second_layer_matrix):
    row_index = jnp.arange(ROWS, dtype=jnp.int32)
    shared_copy = selected_specialists * REPL + (row_index % REPL)[:, None]
    task_copy = SHARED * REPL + query_job_label[:, None] * TASK_EXP + selected_specialists - SHARED
    expert_ids = jnp.where(selected_specialists < SHARED, shared_copy, task_copy).astype(jnp.int32)
    linear_specialist_number = expert_ids.reshape(-1)
    specialist_onehot = (linear_specialist_number[:, None] == jnp.arange(EXPERTS, dtype=jnp.int32)[None, :]).astype(jnp.int32)
    before = jnp.cumsum(specialist_onehot, axis=0) - specialist_onehot
    arrival_rank = jnp.sum(before * specialist_onehot, axis=1).astype(jnp.int32)
    surviving_slot_flags = arrival_rank < copy_room_sizes[linear_specialist_number]
    row_of_entry = (jnp.arange(linear_specialist_number.shape[0], dtype=jnp.int32) // TOP).astype(jnp.int32)

    def one_expert(expert_index):
        target = jnp.where((linear_specialist_number == expert_index) & surviving_slot_flags, arrival_rank, CAPACITY).astype(jnp.int32)
        source = jnp.zeros((CAPACITY,), jnp.int32).at[target].set(row_of_entry, mode="drop")
        live_mask = jnp.zeros((CAPACITY,), jnp.bool_).at[target].set(True, mode="drop")
        block_rows = jnp.where(live_mask[:, None], query_features[source], jnp.zeros((), jnp.bfloat16))
        return expert_mlp(block_rows, first_layer_matrix[expert_index], second_layer_matrix[expert_index])

    outputs = lax.map(one_expert, jnp.arange(EXPERTS, dtype=jnp.int32))
    picked = outputs[linear_specialist_number, jnp.minimum(arrival_rank, CAPACITY - 1)]
    gate_float = whole_number_mixing_factors.astype(jnp.float32)
    gate_share = gate_float / jnp.sum(gate_float, axis=1, keepdims=True)
    row_weight = gate_share.reshape(-1) * surviving_slot_flags.astype(jnp.float32)
    weighted = row_weight[:, None] * picked.astype(jnp.float32)
    return jnp.sum(weighted.reshape(ROWS, TOP, D), axis=1).astype(jnp.bfloat16)
```

```python
import functools

import jax
import jax.numpy as jnp
from jax import lax
from jax.experimental import pallas as pl
from jax.experimental.pallas import tpu as pltpu
from jax.sharding import PartitionSpec as P

TASKS = 8
SHARED = 8
MESH = pl.DeviceIdType.MESH
CHUNKS = 4
FERRIED = ()
OUTER = ('own', 'reply', 'other', 'weigh', 'far0', 'far1')
INNER = ('guest0', 'guest1', 'far0', 'lodge', 'weigh', 'far1', 'back0', 'own', 'reply', 'back1')
LIMIT = 56 * 2**20


def flip(a, b, n):
    total, bit = 0, 1
    while bit < n:
        x, y = (a // bit) % 2, (b // bit) % 2
        total = total + bit * (x + y - 2 * x * y)
        bit *= 2
    return total


def each(lo, hi, fn):
    if hi - lo <= 16:
        for d in range(lo, hi):
            fn(d)
    else:

        @pl.loop(lo, hi)
        def _(d):
            fn(d)


def kernel(
    n,
    slot,
    chunks,
    room_ref,
    label_hbm,
    sel_hbm,
    mix_hbm,
    x_hbm,
    w1_hbm,
    w2_hbm,
    out_hbm,
    label_ref,
    sel_ref,
    mix_ref,
    x_ref,
    out_ref,
    w1,
    w2,
    visits,
    outgoing,
    relayed,
    inbox,
    hidden,
    results,
    returned,
    relay_in,
    home_out,
    home_in,
    partial,
    weights,
    counts,
    route_out,
    route_in,
    transit,
    w_sem,
    in_sem,
    out_sem,
    dense_send,
    pass_send,
    visit_recv,
    route_send,
    route_recv,
    tally_send,
    tally_recv,
    near_send,
    near_recv,
    lodge_send,
    lodge_recv,
    far_send,
    far_recv,
    near_rsend,
    near_rrecv,
    far_rsend,
    far_rrecv,
    back_send,
    back_recv,
    shut_send,
    shut_recv,
):
    me = lax.axis_index("expert")
    group = lax.axis_index("groups")
    lanes = n // 4
    half = 2 * lanes
    mirror = 3 * lanes
    rows, width = x_hbm.shape
    span = half * slot
    cross = lanes // 2
    block = lanes * slot
    part = width // chunks
    hid = w1.shape[1]
    padded = counts.shape[2]
    copies, task_width = n // (2 * SHARED), n // (2 * TASKS)
    plane = me // lanes
    inner = plane // 2 + plane % 2 == 1
    outer = plane // 2 + plane % 2 != 1

    barrier = pltpu.get_barrier_semaphore()

    def peer(d):
        return (group, flip(me, d, n))

    each(
        1,
        n,
        lambda d: pl.semaphore_signal(
            barrier, inc=1, device_id=peer(d), device_id_type=MESH
        ),
    )

    inputs = [
        pltpu.make_async_copy(src, dst, in_sem.at[i])
        for i, (src, dst) in enumerate(
            (
                (label_hbm, label_ref),
                (sel_hbm, sel_ref),
                (mix_hbm, mix_ref),
                (x_hbm, x_ref),
            )
        )
    ]
    for load in inputs:
        load.start()
    load1 = pltpu.make_async_copy(w1_hbm.at[0], w1, w_sem.at[0])
    load2 = pltpu.make_async_copy(w2_hbm.at[0], w2, w_sem.at[1])
    load1.start()
    load2.start()

    def remote(src, dst, send, recv, d):
        return pltpu.make_async_remote_copy(
            src_ref=src,
            dst_ref=dst,
            send_sem=send,
            recv_sem=recv,
            device_id=peer(d),
            device_id_type=MESH,
        )

    def at(first, d, k=None):
        start = first + d * slot
        if not isinstance(start, int):
            start = pl.multiple_of(start, slot)
        if k is None:
            return (pl.ds(start, slot), slice(None))
        return (pl.ds(start, slot), pl.ds(k * part, part))

    def columns(k):
        return (slice(None), pl.ds(k * part, part))

    def tally(d):
        return remote(counts.at[0], counts.at[d], tally_send, tally_recv, d)

    def route(i, j, d):
        return remote(
            route_out.at[i], route_in.at[j], route_send.at[i], route_recv.at[j], d
        )

    def dense(j, d, k):
        return remote(
            x_ref.at[columns(k)],
            visits.at[(j,) + columns(k)],
            dense_send,
            visit_recv.at[j, k],
            d,
        )

    def pass_on(k):
        return remote(
            visits.at[(2,) + columns(k)],
            visits.at[(1,) + columns(k)],
            pass_send,
            visit_recv.at[1, k],
            mirror,
        )

    def near(side, l):
        d = side * lanes + l
        return remote(
            outgoing.at[at(0, d)],
            inbox.at[at(0, d)],
            near_send,
            near_recv.at[side],
            d,
        )

    def lodge(l, k):
        return remote(
            relayed.at[(2,) + at(0, l, k)],
            inbox.at[at(block, l, k)],
            lodge_send,
            lodge_recv,
            l,
        )

    def far(g, side, l, k):
        d = side * lanes + l
        return remote(
            relayed.at[(g,) + at(0, d, k)],
            inbox.at[at((2 + g) * block, l, k)],
            far_send.at[g],
            far_recv.at[g],
            d,
        )

    def near_answer(d):
        return remote(
            results.at[at(0, d)], returned.at[at(0, d)], near_rsend, near_rrecv, d
        )

    def far_answer(g, side, l, k):
        d = side * lanes + l
        return remote(
            results.at[at((2 + g) * block, l, k)],
            relay_in.at[(g,) + at(0, d, k)],
            far_rsend.at[g],
            far_rrecv.at[g, k],
            d,
        )

    def shuttle(g, l, k):
        return remote(
            results.at[at((1 + g) * block, l, k)],
            transit.at[(g,) + at(0, l, k)],
            shut_send.at[g],
            shut_recv.at[g, k],
            l,
        )

    def ferry(g, l, k):
        if g == 0:
            dst, send, recv = returned.at[at(block, l, k)], near_rsend, near_rrecv
        else:
            dst = relay_in.at[(g - 1,) + at(block, l, k)]
            send, recv = far_rsend.at[g - 1], far_rrecv.at[g - 1, k]
        return remote(transit.at[(g,) + at(0, l, k)], dst, send, recv, lanes)

    def back(g, k):
        return remote(
            home_out.at[(g,) + columns(k)],
            home_in.at[columns(k)],
            back_send,
            back_recv.at[k],
            mirror if g == 0 else half,
        )

    def put(k):
        return pltpu.make_async_copy(
            out_ref.at[columns(k)], out_hbm.at[columns(k)], out_sem.at[k]
        )

    def bulk(sem, count, k=None):
        area = inbox.at[pl.ds(0, count * slot)]
        if k is not None:
            area = inbox.at[(pl.ds(0, count * slot), pl.ds(k * part, part))]
        return pltpu.make_async_copy(area, area, sem)

    for load in inputs:
        load.wait()
    lane = lax.broadcasted_iota(jnp.int32, (1, rows), 1)
    task_id = SHARED * copies + label_ref[...] * task_width + sel_ref[0:1, :] - SHARED
    shared_id = sel_ref[1:2, :] * copies + lane % copies
    expert = lax.broadcasted_iota(jnp.int32, (padded, rows), 0)
    task_hot = (expert == task_id).astype(jnp.float32)
    shared_hot = (expert == shared_id).astype(jnp.float32)
    hot = (task_hot + shared_hot).astype(jnp.bfloat16)
    earlier = (
        lax.broadcasted_iota(jnp.int32, (rows, rows), 0)
        < lax.broadcasted_iota(jnp.int32, (rows, rows), 1)
    ).astype(jnp.float32)
    before = jnp.dot(
        hot, earlier.astype(jnp.bfloat16), preferred_element_type=jnp.float32
    )
    task_rank = jnp.sum(before * task_hot, axis=0, keepdims=True)
    shared_rank = jnp.sum(before * shared_hot, axis=0, keepdims=True)
    counts[0] = lax.dot_general(
        jnp.ones((8, rows), jnp.bfloat16),
        hot,
        (((1,), (1,)), ((), ())),
        preferred_element_type=jnp.float32,
    )[:1]

    task_near = (task_id ^ me) < half
    near_id = jnp.where(task_near, task_id, shared_id)
    far_id = jnp.where(task_near, shared_id, task_id)
    near_rank = jnp.where(task_near, task_rank, shared_rank).astype(jnp.int32)
    far_rank = jnp.where(task_near, shared_rank, task_rank).astype(jnp.int32)
    near_slot = (near_id ^ me) * slot + near_rank
    relay = flip(me, half, n) * (1 - inner.astype(jnp.int32)) + flip(
        me, mirror, n
    ) * inner.astype(jnp.int32)
    route_out[0] = (far_id ^ relay) * slot + far_rank
    route_out[1] = (near_id ^ flip(me, lanes, n)) * slot + near_rank

    def choice(slots, count):
        slot_row = lax.broadcasted_iota(jnp.int32, (count, rows), 0)
        return (slot_row == slots).astype(jnp.float32).astype(jnp.bfloat16)

    def pack(chosen, block_rows):
        return jnp.dot(chosen, block_rows, preferred_element_type=jnp.float32).astype(
            jnp.bfloat16
        )

    near_pack = pack(choice(near_slot, span), x_ref[...])
    outgoing[...] = near_pack
    inbox[pl.ds(0, slot)] = near_pack[:slot]

    tile = min(1024, hid)
    out_tile = min(512, width)

    def expand(g):
        @pl.loop(0, hid // tile)
        def _(t):
            cols = pl.ds(pl.multiple_of(t * tile, tile), tile)
            h = jnp.dot(
                inbox[pl.ds(g * block, block)],
                w1[:, cols],
                preferred_element_type=jnp.float32,
            )
            hidden[:, cols] = jax.nn.gelu(h).astype(jnp.bfloat16)

    def shrink(g, cols):
        y = jnp.dot(hidden[...], w2[:, cols], preferred_element_type=jnp.float32)
        results[pl.ds(g * block, block), cols] = y.astype(jnp.bfloat16)

    def near_work(g):
        expand(g)

        @pl.loop(0, width // out_tile)
        def _(t):
            shrink(g, pl.ds(pl.multiple_of(t * out_tile, out_tile), out_tile))

        if g == 0:
            returned[pl.ds(0, slot)] = results[pl.ds(0, slot)]

    def far_work(g, send):
        with jax.named_scope(f'far_expand{g}'):
            expand(2 + g)
        with jax.named_scope(f'far_shrink{g}'):
            pair = min(2, chunks)
            for j in range(chunks // pair):
                shrink(2 + g, pl.ds(j * pair * part, pair * part))
                for k in range(j * pair, (j + 1) * pair):
                    send(k)

    def ferry_all(g):
        for k in range(chunks):
            bulk(shut_recv.at[g, k], lanes - cross, k).wait()
            each(cross, lanes, lambda l: ferry(g, l, k).start())

    def column(row):
        return jnp.broadcast_to(row, (128, row.shape[1])).T[:, :1]

    def reader(slots):
        slot_lane = lax.broadcasted_iota(jnp.int32, (rows, span), 1).astype(jnp.float32)
        slots = column(slots.astype(jnp.float32))
        return (slot_lane == slots).astype(jnp.float32).astype(jnp.bfloat16)

    def weigh():
        pltpu.make_async_copy(counts.at[pl.ds(1, n - 1)], counts.at[pl.ds(1, n - 1)], tally_recv).wait()
        offset = jnp.zeros((1, padded), jnp.float32)
        for d in range(1, n):
            offset = offset + counts[d] * jnp.where(flip(me, d, n) < me, 1.0, 0.0)
        offset = column(offset)
        arrival_task = task_rank + jnp.sum(task_hot * offset, axis=0, keepdims=True)
        arrival_shared = shared_rank + jnp.sum(
            shared_hot * offset, axis=0, keepdims=True
        )
        room_task = jnp.zeros((1, rows), jnp.int32)
        room_shared = jnp.zeros((1, rows), jnp.int32)
        for e in range(n):
            size = room_ref[e]
            if e < half:
                room_shared = jnp.where(shared_id == e, size, room_shared)
            else:
                room_task = jnp.where(task_id == e, size, room_task)
        keep_task = (arrival_task < room_task.astype(jnp.float32)).astype(jnp.float32)
        keep_shared = (arrival_shared < room_shared.astype(jnp.float32)).astype(
            jnp.float32
        )
        mix = mix_ref[...].astype(jnp.float32)
        total = mix[0:1] + mix[1:2]
        task_weight = mix[0:1] / total * keep_task
        shared_weight = mix[1:2] / total * keep_shared
        weights[0] = column(jnp.where(task_near, task_weight, shared_weight))
        weights[1] = column(jnp.where(task_near, shared_weight, task_weight))

    with jax.named_scope('barrier'):
        pl.semaphore_wait(barrier, n - 1)

    @pl.when(outer)
    def _():
        for k in range(chunks):
            dense(2, lanes, k).start()
            if k == 0:
                route(1, 2, lanes).start()
                route(0, 1, half).start()
        each(1, lanes, lambda l: near(0, l).start())
        each(1, n, lambda d: tally(d).start())

        def own():
            with jax.named_scope('o_wait_own'):
                load1.wait()
                load2.wait()
                bulk(near_recv.at[0], lanes - 1).wait()
            with jax.named_scope('o_work0'):
                near_work(0)

        def reply():
            each(1, lanes, lambda d: near_answer(d).start())

        def other():
            with jax.named_scope('o_wait_other'):
                bulk(near_recv.at[1], lanes).wait()
            with jax.named_scope('o_work1'):
                near_work(1)
            if 0 in FERRIED:
                for k in range(chunks):
                    each(cross, lanes, lambda l: shuttle(0, l, k).start())
                each(0, cross, lambda l: near_answer(lanes + l).start())
            else:
                each(lanes, half, lambda d: near_answer(d).start())

        def await_far(g):
            with jax.named_scope(f'o_far_wait{g}'):
                bulk(far_recv.at[g], lanes).wait()

        def far_step(g):
            def send(k):
                if 1 + g in FERRIED:
                    each(cross, lanes, lambda l: shuttle(1 + g, l, k).start())
                    each(0, cross, lambda l: far_answer(g, 1, l, k).start())
                else:
                    each(0, lanes, lambda l: far_answer(g, 1, l, k).start())

            far_work(g, send)

        def carry(g):
            with jax.named_scope(f'o_ferry{g}'):
                ferry_all(g)

        def weigh_step():
            with jax.named_scope('o_weigh'):
                weigh()

        steps = {"own": own, "reply": reply, "other": other, "weigh": weigh_step}
        for g in range(2):
            steps[f"await{g}"] = functools.partial(await_far, g)
            steps[f"far{g}"] = functools.partial(far_step, g)
        for g in range(3):
            steps[f"ferry{g}"] = functools.partial(carry, g)
        if "await1" not in OUTER:
            steps["far1"] = lambda: (await_far(1), far_step(1))
        steps["far0"] = lambda: (await_far(0), far_step(0))
        for step in OUTER:
            steps[step]()

    @pl.when(inner)
    def _():
        for k in range(chunks):
            dense(0, mirror, k).start()
            if k == 0:
                route(0, 0, mirror).start()
        each(0, lanes, lambda l: near(1, l).start())
        each(1, lanes, lambda l: near(0, l).start())
        each(1, n, lambda d: tally(d).start())

        def host(g, chosen, k):
            packed = pack(chosen, visits[(g,) + columns(k)])
            relayed[(g, slice(None), pl.ds(k * part, part))] = packed
            inbox[at((2 + g) * block, 0, k)] = packed[:slot]
            each(1, lanes, lambda l: far(g, 0, l, k).start())
            each(0, lanes, lambda l: far(g, 1, l, k).start())

        def guest0():
            route(1, 2, lanes).wait_recv()
            route(0, 0, mirror).wait_recv()
            lodge_choice = choice(route_in[2], block)
            guest_choice = choice(route_in[0], span)
            for k in range(chunks):
                with jax.named_scope(f'i_waitG{k}'):
                    dense(2, lanes, k).wait_recv()
                pass_on(k).start()
                with jax.named_scope(f'i_waitg0_{k}'):
                    dense(0, mirror, k).wait_recv()
                with jax.named_scope(f'i_host0_{k}'):
                    host(0, guest_choice, k)
                packed = pack(lodge_choice, visits[(2,) + columns(k)])
                relayed[(2, pl.ds(0, block), pl.ds(k * part, part))] = packed
                inbox[at(block, 0, k)] = packed[:slot]
                each(1, lanes, lambda l: lodge(l, k).start())
            load1.wait()
            load2.wait()

        def own():
            with jax.named_scope('i_wait_own'):
                bulk(near_recv.at[0], lanes - 1).wait()
            with jax.named_scope('i_work0'):
                near_work(0)

        def reply():
            each(1, lanes, lambda d: near_answer(d).start())

        def guest1():
            route(0, 1, half).wait_recv()
            guest_choice = choice(route_in[1], span)
            for k in range(chunks):
                with jax.named_scope(f'i_waitg1_{k}'):
                    pass_on(k).wait_recv()
                with jax.named_scope(f'i_host1_{k}'):
                    host(1, guest_choice, k)

        def lodged():
            with jax.named_scope('i_waitlodge'):
                bulk(lodge_recv, lanes - 1).wait()
            with jax.named_scope('i_work1'):
                near_work(1)
            each(lanes, half, lambda d: near_answer(d).start())

        def take_back(g, lo, hi):
            guest_reader = reader(route_in[g])
            for k in range(lo, hi):
                with jax.named_scope(f'i_waitans{g}_{k}'):
                    bulk(far_rrecv.at[g, k], half - 1, k).wait()
                home_out[(g,) + columns(k)] = pack(
                    guest_reader, relay_in[(g, slice(None), pl.ds(k * part, part))]
                )
                back(g, k).start()

        def far_step(g):
            def send(k):
                each(1, lanes, lambda l: far_answer(g, 0, l, k).start())
                relay_in[(g,) + at(0, 0, k)] = results[at((2 + g) * block, 0, k)]

            with jax.named_scope(f'i_far_wait{g}'):
                bulk(far_recv.at[g], lanes - 1).wait()
            far_work(g, send)

        def weigh_step():
            with jax.named_scope('i_weigh'):
                weigh()

        steps = {"own": own, "reply": reply, "guest0": guest0, "guest1": guest1, "lodge": lodged, "weigh": weigh_step}
        for g in range(2):
            steps[f"far{g}"] = functools.partial(far_step, g)
            steps[f"back{g}"] = functools.partial(take_back, g, 0, chunks)
            steps[f"back{g}a"] = functools.partial(take_back, g, 0, chunks // 2)
            steps[f"back{g}b"] = functools.partial(take_back, g, chunks // 2, chunks)
        for step in INNER:
            steps[step]()

    near_reader = reader(near_slot)
    with jax.named_scope('wait_near_ans'):
        bulk(near_rrecv, half - 1).wait()
    partial[...] = (
        jnp.dot(near_reader, returned[...], preferred_element_type=jnp.float32)
        * weights[0]
    )
    far_weight = weights[1]
    for k in range(chunks):
        with jax.named_scope(f'wait_back{k}'):
            back(0, k).wait_recv()
        out_ref[columns(k)] = (
            partial[columns(k)] + home_in[columns(k)].astype(jnp.float32) * far_weight
        ).astype(jnp.bfloat16)
        put(k).start()

    with jax.named_scope('drain'):
        pltpu.make_async_copy(
            counts.at[pl.ds(1, n - 1)], counts.at[pl.ds(1, n - 1)], tally_send
        ).wait()
        bulk(near_rsend, half - 1).wait()
        route(0, 0, mirror).wait_send()
        pltpu.make_async_copy(x_ref, home_in, dense_send).wait()

        @pl.when(outer)
        def _():
            route(1, 2, lanes).wait_send()
            bulk(near_send, lanes - 1).wait()
            for g in range(2):
                bulk(far_rsend.at[g], lanes).wait()
            for g in FERRIED:
                bulk(shut_send.at[g], lanes - cross).wait()

        @pl.when(inner)
        def _():
            bulk(near_send, half - 1).wait()
            pltpu.make_async_copy(x_ref, home_in, pass_send).wait()
            bulk(lodge_send, lanes - 1).wait()
            for g in range(2):
                bulk(far_send.at[g], half - 1).wait()
                bulk(far_rsend.at[g], lanes - 1).wait()
            pltpu.make_async_copy(home_out, home_out, back_send).wait()

        for k in range(chunks):
            put(k).wait()


def solution(mesh):
    n = mesh.shape["expert"]

    def shards(x, label, sel, mix, room, first, second):
        rows, width = x.shape
        hid = first.shape[2]
        slot = -(-(4 * rows // n) // 16) * 16
        lanes, half = n // 4, n // 2
        chunks = CHUNKS if lanes <= 8 else 1
        padded = -(-n // 128) * 128
        bf16, f32, i32 = jnp.bfloat16, jnp.float32, jnp.int32
        anywhere = pl.BlockSpec(memory_space=pltpu.HBM)
        dma = pltpu.SemaphoreType.DMA
        return pl.pallas_call(
            functools.partial(kernel, n, slot, chunks),
            out_shape=jax.ShapeDtypeStruct((rows, width), bf16),
            in_specs=[pl.BlockSpec(memory_space=pltpu.SMEM)]
            + [anywhere] * 6,
            out_specs=anywhere,
            scratch_shapes=[
                pltpu.VMEM((1, rows), i32),
                pltpu.VMEM((2, rows), i32),
                pltpu.VMEM((2, rows), i32),
                pltpu.VMEM((rows, width), bf16),
                pltpu.VMEM((rows, width), bf16),
                pltpu.VMEM(first.shape[1:], bf16),
                pltpu.VMEM(second.shape[1:], bf16),
                pltpu.VMEM((3, rows, width), bf16),
                pltpu.VMEM((half * slot, width), bf16),
                pltpu.VMEM((3, half * slot, width), bf16),
                pltpu.VMEM((n * slot, width), bf16),
                pltpu.VMEM((lanes * slot, hid), bf16),
                pltpu.VMEM((n * slot, width), bf16),
                pltpu.VMEM((half * slot, width), bf16),
                pltpu.VMEM((2, half * slot, width), bf16),
                pltpu.VMEM((2, rows, width), bf16),
                pltpu.VMEM((rows, width), bf16),
                pltpu.VMEM((rows, width), f32),
                pltpu.VMEM((2, rows, 1), f32),
                pltpu.VMEM((n, 1, padded), f32),
                pltpu.VMEM((2, 1, rows), i32),
                pltpu.VMEM((3, 1, rows), i32),
                pltpu.VMEM((3, lanes * slot, width), bf16),
                dma((2,)),
                dma((4,)),
                dma((chunks,)),
                dma(()),
                dma(()),
                dma((3, chunks)),
                dma((2,)),
                dma((3,)),
                dma(()),
                dma(()),
                dma(()),
                dma((2,)),
                dma(()),
                dma(()),
                dma((2,)),
                dma((2,)),
                dma(()),
                dma(()),
                dma((2,)),
                dma((2, chunks)),
                dma(()),
                dma((chunks,)),
                dma((3,)),
                dma((3, chunks)),
            ],
            compiler_params=pltpu.CompilerParams(
                collective_id=0, has_side_effects=True, vmem_limit_bytes=LIMIT
            ),
        )(room, label.reshape(1, rows), sel.T, mix.T, x, first, second)

    in_specs = (
        P(("groups", "expert"), None),
        P(("groups", "expert")),
        P(("groups", "expert"), None),
        P(("groups", "expert"), None),
        P(),
        P("expert", None, None),
        P("expert", None, None),
    )
    return jax.shard_map(
        shards,
        mesh=mesh,
        in_specs=in_specs,
        out_specs=P(("groups", "expert"), None),
        check_vma=False,
    )
```

```python
import functools

import jax
import jax.numpy as jnp
from jax import lax
from jax.experimental import pallas as pl
from jax.experimental.pallas import tpu as pltpu
from jax.sharding import PartitionSpec as P

TASKS = 8
SHARED = 8
MESH = pl.DeviceIdType.MESH
CHUNKS = 4
OUTER = ('other0', 'own', 'far0', 'reply', 'far1', 'other1', 'weigh')
INNER = ('guest0', 'own', 'guest1', 'far0', 'lodge', 'far1', 'reply', 'back0', 'weigh', 'back1')
LIMIT = 56 * 2**20


def flip(a, b, n):
    total, bit = 0, 1
    while bit < n:
        x, y = (a // bit) % 2, (b // bit) % 2
        total = total + bit * (x + y - 2 * x * y)
        bit *= 2
    return total


def each(lo, hi, fn):
    if hi - lo <= 16:
        for d in range(lo, hi):
            fn(d)
    else:

        @pl.loop(lo, hi)
        def _(d):
            fn(d)


def kernel(
    n,
    slot,
    chunks,
    room_ref,
    label_hbm,
    sel_hbm,
    mix_hbm,
    x_hbm,
    w1_hbm,
    w2_hbm,
    out_hbm,
    label_ref,
    sel_ref,
    mix_ref,
    x_ref,
    out_ref,
    w1,
    w2,
    visits,
    outgoing,
    relayed,
    inbox,
    hidden,
    results,
    returned,
    relay_in,
    home_out,
    home_in,
    partial,
    weights,
    counts,
    route_out,
    route_in,
    w_sem,
    in_sem,
    out_sem,
    dense_send,
    pass_send,
    visit_recv,
    route_send,
    route_recv,
    tally_send,
    tally_recv,
    near_send,
    near_recv,
    lodge_send,
    lodge_recv,
    far_send,
    far_recv,
    near_rsend,
    near_rrecv,
    far_rsend,
    far_rrecv,
    back_send,
    back_recv,
):
    me = lax.axis_index("expert")
    group = lax.axis_index("groups")
    lanes = n // 4
    half = 2 * lanes
    mirror = 3 * lanes
    rows, width = x_hbm.shape
    span = half * slot
    cross = lanes // 2
    block = lanes * slot
    part = width // chunks
    hid = w1.shape[1]
    padded = counts.shape[2]
    copies, task_width = n // (2 * SHARED), n // (2 * TASKS)
    plane = me // lanes
    inner = plane // 2 + plane % 2 == 1
    outer = plane // 2 + plane % 2 != 1

    barrier = pltpu.get_barrier_semaphore()

    def peer(d):
        return (group, flip(me, d, n))

    with jax.named_scope('signals'):
        each(
            1,
            n,
            lambda d: pl.semaphore_signal(
                barrier, inc=1, device_id=peer(d), device_id_type=MESH
            ),
        )

    inputs = [
        pltpu.make_async_copy(src, dst, in_sem.at[i])
        for i, (src, dst) in enumerate(
            (
                (label_hbm, label_ref),
                (sel_hbm, sel_ref),
                (mix_hbm, mix_ref),
                (x_hbm, x_ref),
            )
        )
    ]
    for load in inputs:
        load.start()
    load1 = pltpu.make_async_copy(w1_hbm.at[0], w1, w_sem.at[0])
    load2 = pltpu.make_async_copy(w2_hbm.at[0], w2, w_sem.at[1])

    def remote(src, dst, send, recv, d):
        return pltpu.make_async_remote_copy(
            src_ref=src,
            dst_ref=dst,
            send_sem=send,
            recv_sem=recv,
            device_id=peer(d),
            device_id_type=MESH,
        )

    def at(first, d, k=None):
        start = first + d * slot
        if not isinstance(start, int):
            start = pl.multiple_of(start, slot)
        if k is None:
            return (pl.ds(start, slot), slice(None))
        return (pl.ds(start, slot), pl.ds(k * part, part))

    def columns(k):
        return (slice(None), pl.ds(k * part, part))

    def tally(d):
        return remote(counts.at[0], counts.at[d], tally_send, tally_recv, d)

    def route(i, j, d):
        return remote(
            route_out.at[i], route_in.at[j], route_send.at[i], route_recv.at[j], d
        )

    def dense(j, d, k):
        return remote(
            x_ref.at[columns(k)],
            visits.at[(j,) + columns(k)],
            dense_send,
            visit_recv.at[j, k],
            d,
        )

    def pass_on(k):
        return remote(
            visits.at[(2,) + columns(k)],
            visits.at[(1,) + columns(k)],
            pass_send,
            visit_recv.at[1, k],
            mirror,
        )

    def near(side, l, part=0):
        d = side * lanes + l
        return remote(
            outgoing.at[at(0, d)],
            inbox.at[at(0, d)],
            near_send,
            near_recv.at[side + part],
            d,
        )

    def lodge(l, k):
        return remote(
            relayed.at[(2,) + at(0, l, k)],
            inbox.at[at(block, l, k)],
            lodge_send,
            lodge_recv,
            l,
        )

    def far(g, side, l, k):
        d = side * lanes + l
        return remote(
            relayed.at[(g,) + at(0, d, k)],
            inbox.at[at((2 + g) * block, l, k)],
            far_send.at[g],
            far_recv.at[g],
            d,
        )

    def near_answer(d):
        return remote(
            results.at[at(0, d)], returned.at[at(0, d)], near_rsend, near_rrecv, d
        )

    def far_answer(g, side, l, k):
        d = side * lanes + l
        return remote(
            results.at[at((2 + g) * block, l, k)],
            relay_in.at[(g,) + at(0, d, k)],
            far_rsend.at[g],
            far_rrecv.at[g, k],
            d,
        )

    def back(g, k):
        return remote(
            home_out.at[(g,) + columns(k)],
            home_in.at[columns(k)],
            back_send,
            back_recv.at[k],
            mirror if g == 0 else half,
        )

    def put(k):
        return pltpu.make_async_copy(
            out_ref.at[columns(k)], out_hbm.at[columns(k)], out_sem.at[k]
        )

    def bulk(sem, count, k=None):
        area = inbox.at[pl.ds(0, count * slot)]
        if k is not None:
            area = inbox.at[(pl.ds(0, count * slot), pl.ds(k * part, part))]
        return pltpu.make_async_copy(area, area, sem)

    def enter():
        with jax.named_scope('barrier'):
            pl.semaphore_wait(barrier, n - 1)

    def send_rows():
        route(1, 2, lanes).start()
        route(0, 1, half).start()
        for k in range(chunks):
            dense(2, lanes, k).start()

    with jax.named_scope('wait_small'):
        for load in inputs[:3]:
            load.wait()
    lane = lax.broadcasted_iota(jnp.int32, (1, rows), 1)
    task_id = SHARED * copies + label_ref[...] * task_width + sel_ref[0:1, :] - SHARED
    shared_id = sel_ref[1:2, :] * copies + lane % copies
    expert = lax.broadcasted_iota(jnp.int32, (padded, rows), 0)
    task_hot = (expert == task_id).astype(jnp.float32)
    shared_hot = (expert == shared_id).astype(jnp.float32)
    hot = (task_hot + shared_hot).astype(jnp.bfloat16)
    earlier = (
        lax.broadcasted_iota(jnp.int32, (rows, rows), 0)
        < lax.broadcasted_iota(jnp.int32, (rows, rows), 1)
    ).astype(jnp.float32)
    before = jnp.dot(
        hot, earlier.astype(jnp.bfloat16), preferred_element_type=jnp.float32
    )
    task_rank = jnp.sum(before * task_hot, axis=0, keepdims=True)
    shared_rank = jnp.sum(before * shared_hot, axis=0, keepdims=True)
    counts[0] = lax.dot_general(
        jnp.ones((8, rows), jnp.bfloat16),
        hot,
        (((1,), (1,)), ((), ())),
        preferred_element_type=jnp.float32,
    )[:1]

    task_near = (task_id ^ me) < half
    near_id = jnp.where(task_near, task_id, shared_id)
    far_id = jnp.where(task_near, shared_id, task_id)
    near_rank = jnp.where(task_near, task_rank, shared_rank).astype(jnp.int32)
    far_rank = jnp.where(task_near, shared_rank, task_rank).astype(jnp.int32)
    near_slot = (near_id ^ me) * slot + near_rank
    relay = flip(me, half, n) * (1 - inner.astype(jnp.int32)) + flip(
        me, mirror, n
    ) * inner.astype(jnp.int32)
    route_out[0] = (far_id ^ relay) * slot + far_rank
    route_out[1] = (near_id ^ flip(me, lanes, n)) * slot + near_rank

    @pl.when(plane == 3)
    def _():
        with jax.named_scope('wait_x'):
            inputs[3].wait()
        enter()
        send_rows()
        load1.start()
        load2.start()

    @pl.when(plane != 3)
    def _():
        inputs[3].wait()
        load1.start()
        load2.start()

    def choice(slots, count):
        slot_row = lax.broadcasted_iota(jnp.int32, (count, rows), 0)
        return (slot_row == slots).astype(jnp.float32).astype(jnp.bfloat16)

    def pack(chosen, block_rows):
        return jnp.dot(chosen, block_rows, preferred_element_type=jnp.float32).astype(
            jnp.bfloat16
        )

    with jax.named_scope('near_pack'):
        near_pack = pack(choice(near_slot, span), x_ref[...])
        outgoing[...] = near_pack
        inbox[pl.ds(0, slot)] = near_pack[:slot]

    tile = hid
    out_tile = min(512, width)

    def expand(first, count):
        @pl.loop(0, hid // tile)
        def _(t):
            cols = pl.ds(pl.multiple_of(t * tile, tile), tile)
            h = jnp.dot(
                inbox[pl.ds(first, count)],
                w1[:, cols],
                preferred_element_type=jnp.float32,
            )
            hidden[:count, cols] = jax.nn.gelu(h).astype(jnp.bfloat16)

    def shrink(first, count, cols):
        y = jnp.dot(
            hidden[:count], w2[:, cols], preferred_element_type=jnp.float32
        )
        results[pl.ds(first, count), cols] = y.astype(jnp.bfloat16)

    def near_work(first, count):
        expand(first, count)

        @pl.loop(0, width // out_tile)
        def _(t):
            cols = pl.ds(pl.multiple_of(t * out_tile, out_tile), out_tile)
            shrink(first, count, cols)

        if first == 0:
            returned[pl.ds(0, slot)] = results[pl.ds(0, slot)]

    def far_work(g, send):
        with jax.named_scope(f'far_expand{g}'):
            expand((2 + g) * block, block)
        with jax.named_scope(f'far_shrink{g}'):
            pair = min(4, chunks)
            for j in range(chunks // pair):
                shrink((2 + g) * block, block, pl.ds(j * pair * part, pair * part))
                for k in range(j * pair, (j + 1) * pair):
                    send(k)

    def column(row):
        return jnp.broadcast_to(row, (128, row.shape[1])).T[:, :1]

    def reader(slots):
        slot_lane = lax.broadcasted_iota(jnp.int32, (rows, span), 1).astype(jnp.float32)
        slots = column(slots.astype(jnp.float32))
        return (slot_lane == slots).astype(jnp.float32).astype(jnp.bfloat16)

    def weigh():
        pltpu.make_async_copy(counts.at[pl.ds(1, n - 1)], counts.at[pl.ds(1, n - 1)], tally_recv).wait()
        offset = jnp.zeros((1, padded), jnp.float32)
        for d in range(1, n):
            offset = offset + counts[d] * jnp.where(flip(me, d, n) < me, 1.0, 0.0)
        offset = column(offset)
        arrival_task = task_rank + jnp.sum(task_hot * offset, axis=0, keepdims=True)
        arrival_shared = shared_rank + jnp.sum(
            shared_hot * offset, axis=0, keepdims=True
        )
        room_task = jnp.zeros((1, rows), jnp.int32)
        room_shared = jnp.zeros((1, rows), jnp.int32)
        for e in range(n):
            size = room_ref[e]
            if e < half:
                room_shared = jnp.where(shared_id == e, size, room_shared)
            else:
                room_task = jnp.where(task_id == e, size, room_task)
        keep_task = (arrival_task < room_task.astype(jnp.float32)).astype(jnp.float32)
        keep_shared = (arrival_shared < room_shared.astype(jnp.float32)).astype(
            jnp.float32
        )
        mix = mix_ref[...].astype(jnp.float32)
        total = mix[0:1] + mix[1:2]
        task_weight = mix[0:1] / total * keep_task
        shared_weight = mix[1:2] / total * keep_shared
        weights[0] = column(jnp.where(task_near, task_weight, shared_weight))
        weights[1] = column(jnp.where(task_near, shared_weight, task_weight))

    @pl.when(plane != 3)
    def _():
        enter()

    @pl.when(outer)
    def _():
        @pl.when(plane == 0)
        def _():
            send_rows()

        each(1, lanes, lambda l: near(0, l).start())
        each(1, n, lambda d: tally(d).start())

        def own():
            with jax.named_scope('o_wait_own'):
                bulk(near_recv.at[0], lanes - 1).wait()
            with jax.named_scope('o_work0'):
                near_work(0, block)

        def reply():
            each(1, lanes, lambda d: near_answer(d).start())

        def other(lo, hi, part):
            with jax.named_scope(f'o_wait_other{part}'):
                bulk(near_recv.at[1 + part], hi - lo).wait()
            with jax.named_scope(f'o_work1{part}'):
                near_work(block + lo * slot, (hi - lo) * slot)
            each(lanes + lo, lanes + hi, lambda d: near_answer(d).start())

        def far_step(g):
            def send(k):
                each(0, lanes, lambda l: far_answer(g, 1, l, k).start())

            with jax.named_scope(f'o_far_wait{g}'):
                bulk(far_recv.at[g], lanes).wait()
            far_work(g, send)

        def weigh_step():
            with jax.named_scope('o_weigh'):
                weigh()

        steps = {"own": own, "reply": reply, "other0": functools.partial(other, 0, cross, 0), "other1": functools.partial(other, cross, lanes, 1), "weigh": weigh_step}
        for g in range(2):
            steps[f"far{g}"] = functools.partial(far_step, g)
        load1.wait()
        load2.wait()
        for step in OUTER:
            steps[step]()

    @pl.when(inner)
    def _():
        route(0, 0, mirror).start()
        for k in range(chunks):
            dense(0, mirror, k).start()
        each(0, cross, lambda l: near(1, l).start())
        each(1, lanes, lambda l: near(0, l).start())
        each(1, n, lambda d: tally(d).start())

        def host(g, chosen, k):
            packed = pack(chosen, visits[(g,) + columns(k)])
            relayed[(g, slice(None), pl.ds(k * part, part))] = packed
            inbox[at((2 + g) * block, 0, k)] = packed[:slot]
            each(1, lanes, lambda l: far(g, 0, l, k).start())
            each(0, lanes, lambda l: far(g, 1, l, k).start())

        def guest0():
            route(1, 2, lanes).wait_recv()
            route(0, 0, mirror).wait_recv()
            lodge_choice = choice(route_in[2], block)
            guest_choice = choice(route_in[0], span)
            for k in range(chunks):
                with jax.named_scope(f'i_waitG{k}'):
                    dense(2, lanes, k).wait_recv()
                pass_on(k).start()
                with jax.named_scope(f'i_waitg0_{k}'):
                    dense(0, mirror, k).wait_recv()
                with jax.named_scope(f'i_host0_{k}'):
                    host(0, guest_choice, k)
                packed = pack(lodge_choice, visits[(2,) + columns(k)])
                relayed[(2, pl.ds(0, block), pl.ds(k * part, part))] = packed
                inbox[at(block, 0, k)] = packed[:slot]
                each(1, lanes, lambda l: lodge(l, k).start())
            load1.wait()
            load2.wait()

        def own():
            with jax.named_scope('i_wait_own'):
                bulk(near_recv.at[0], lanes - 1).wait()
            with jax.named_scope('i_work0'):
                near_work(0, block)

        def reply():
            each(1, lanes, lambda d: near_answer(d).start())

        def guest1():
            route(0, 1, half).wait_recv()
            guest_choice = choice(route_in[1], span)
            for k in range(chunks):
                with jax.named_scope(f'i_waitg1_{k}'):
                    pass_on(k).wait_recv()
                with jax.named_scope(f'i_host1_{k}'):
                    host(1, guest_choice, k)
            each(cross, lanes, lambda l: near(1, l, 1).start())

        def lodged():
            with jax.named_scope('i_waitlodge'):
                bulk(lodge_recv, lanes - 1).wait()
            with jax.named_scope('i_work1'):
                near_work(block, block)
            each(lanes, half, lambda d: near_answer(d).start())

        def take_back(g, lo, hi):
            guest_reader = reader(route_in[g])
            for k in range(lo, hi):
                with jax.named_scope(f'i_waitans{g}_{k}'):
                    bulk(far_rrecv.at[g, k], half - 1, k).wait()
                home_out[(g,) + columns(k)] = pack(
                    guest_reader, relay_in[(g, slice(None), pl.ds(k * part, part))]
                )
                back(g, k).start()

        def far_step(g):
            def send(k):
                each(1, lanes, lambda l: far_answer(g, 0, l, k).start())
                relay_in[(g,) + at(0, 0, k)] = results[at((2 + g) * block, 0, k)]

            with jax.named_scope(f'i_far_wait{g}'):
                bulk(far_recv.at[g], lanes - 1).wait()
            far_work(g, send)

        def weigh_step():
            with jax.named_scope('i_weigh'):
                weigh()

        steps = {"own": own, "reply": reply, "guest0": guest0, "guest1": guest1, "lodge": lodged, "weigh": weigh_step}
        for g in range(2):
            steps[f"far{g}"] = functools.partial(far_step, g)
            steps[f"back{g}"] = functools.partial(take_back, g, 0, chunks)
            steps[f"back{g}a"] = functools.partial(take_back, g, 0, chunks // 2)
            steps[f"back{g}b"] = functools.partial(take_back, g, chunks // 2, chunks)
        for step in INNER:
            steps[step]()

    near_reader = reader(near_slot)
    with jax.named_scope('wait_near_ans'):
        bulk(near_rrecv, half - 1).wait()
    partial[...] = (
        jnp.dot(near_reader, returned[...], preferred_element_type=jnp.float32)
        * weights[0]
    )
    far_weight = weights[1]
    for k in range(chunks):
        with jax.named_scope(f'wait_back{k}'):
            back(0, k).wait_recv()
        out_ref[columns(k)] = (
            partial[columns(k)] + home_in[columns(k)].astype(jnp.float32) * far_weight
        ).astype(jnp.bfloat16)
        put(k).start()

    with jax.named_scope('drain'):
        pltpu.make_async_copy(
            counts.at[pl.ds(1, n - 1)], counts.at[pl.ds(1, n - 1)], tally_send
        ).wait()
        bulk(near_rsend, half - 1).wait()
        route(0, 0, mirror).wait_send()
        pltpu.make_async_copy(x_ref, home_in, dense_send).wait()

        @pl.when(outer)
        def _():
            route(1, 2, lanes).wait_send()
            bulk(near_send, lanes - 1).wait()
            for g in range(2):
                bulk(far_rsend.at[g], lanes).wait()

        @pl.when(inner)
        def _():
            bulk(near_send, half - 1).wait()
            pltpu.make_async_copy(x_ref, home_in, pass_send).wait()
            bulk(lodge_send, lanes - 1).wait()
            for g in range(2):
                bulk(far_send.at[g], half - 1).wait()
                bulk(far_rsend.at[g], lanes - 1).wait()
            pltpu.make_async_copy(home_out, home_out, back_send).wait()

        for k in range(chunks):
            put(k).wait()


def solution(mesh):
    n = mesh.shape["expert"]

    def shards(x, label, sel, mix, room, first, second):
        rows, width = x.shape
        hid = first.shape[2]
        slot = -(-(4 * rows // n) // 16) * 16
        lanes, half = n // 4, n // 2
        chunks = CHUNKS if lanes <= 8 else 1
        padded = -(-n // 128) * 128
        bf16, f32, i32 = jnp.bfloat16, jnp.float32, jnp.int32
        anywhere = pl.BlockSpec(memory_space=pltpu.HBM)
        dma = pltpu.SemaphoreType.DMA
        return pl.pallas_call(
            functools.partial(kernel, n, slot, chunks),
            out_shape=jax.ShapeDtypeStruct((rows, width), bf16),
            in_specs=[pl.BlockSpec(memory_space=pltpu.SMEM)]
            + [anywhere] * 6,
            out_specs=anywhere,
            scratch_shapes=[
                pltpu.VMEM((1, rows), i32),
                pltpu.VMEM((2, rows), i32),
                pltpu.VMEM((2, rows), i32),
                pltpu.VMEM((rows, width), bf16),
                pltpu.VMEM((rows, width), bf16),
                pltpu.VMEM(first.shape[1:], bf16),
                pltpu.VMEM(second.shape[1:], bf16),
                pltpu.VMEM((3, rows, width), bf16),
                pltpu.VMEM((half * slot, width), bf16),
                pltpu.VMEM((3, half * slot, width), bf16),
                pltpu.VMEM((n * slot, width), bf16),
                pltpu.VMEM((lanes * slot, hid), bf16),
                pltpu.VMEM((n * slot, width), bf16),
                pltpu.VMEM((half * slot, width), bf16),
                pltpu.VMEM((2, half * slot, width), bf16),
                pltpu.VMEM((2, rows, width), bf16),
                pltpu.VMEM((rows, width), bf16),
                pltpu.VMEM((rows, width), f32),
                pltpu.VMEM((2, rows, 1), f32),
                pltpu.VMEM((n, 1, padded), f32),
                pltpu.VMEM((2, 1, rows), i32),
                pltpu.VMEM((3, 1, rows), i32),
                dma((2,)),
                dma((4,)),
                dma((chunks,)),
                dma(()),
                dma(()),
                dma((3, chunks)),
                dma((2,)),
                dma((3,)),
                dma(()),
                dma(()),
                dma(()),
                dma((3,)),
                dma(()),
                dma(()),
                dma((2,)),
                dma((2,)),
                dma(()),
                dma(()),
                dma((2,)),
                dma((2, chunks)),
                dma(()),
                dma((chunks,)),
            ],
            compiler_params=pltpu.CompilerParams(
                collective_id=0, has_side_effects=True, vmem_limit_bytes=LIMIT
            ),
        )(room, label.reshape(1, rows), sel.T, mix.T, x, first, second)

    in_specs = (
        P(("groups", "expert"), None),
        P(("groups", "expert")),
        P(("groups", "expert"), None),
        P(("groups", "expert"), None),
        P(),
        P("expert", None, None),
        P("expert", None, None),
    )
    return jax.shard_map(
        shards,
        mesh=mesh,
        in_specs=in_specs,
        out_specs=P(("groups", "expert"), None),
        check_vma=False,
    )
```

```python
import functools

import jax
import jax.numpy as jnp
from jax import lax
from jax.experimental import pallas as pl
from jax.experimental.pallas import tpu as pltpu
from jax.sharding import PartitionSpec as P

TASKS = 8
SHARED = 8
MESH = pl.DeviceIdType.MESH
CHUNKS = 4
OUTER = ('other0', 'own', 'far0', 'reply', 'far1', 'other1', 'weigh')
INNER = ('guest0', 'own', 'guest1', 'far0', 'lodge', 'far1', 'reply', 'back0', 'weigh', 'back1')
LIMIT = 56 * 2**20


def flip(a, b, n):
    total, bit = 0, 1
    while bit < n:
        x, y = (a // bit) % 2, (b // bit) % 2
        total = total + bit * (x + y - 2 * x * y)
        bit *= 2
    return total


def each(lo, hi, fn):
    if hi - lo <= 16:
        for d in range(lo, hi):
            fn(d)
    else:

        @pl.loop(lo, hi)
        def _(d):
            fn(d)


def kernel(
    n,
    slot,
    chunks,
    room_hbm,
    label_hbm,
    sel_hbm,
    mix_hbm,
    x_hbm,
    w1_hbm,
    w2_hbm,
    out_hbm,
    room_ref,
    label_ref,
    sel_ref,
    mix_ref,
    x_ref,
    out_ref,
    w1,
    w2,
    visits,
    outgoing,
    relayed,
    inbox,
    hidden,
    results,
    returned,
    relay_in,
    home_out,
    home_in,
    partial,
    weights,
    counts,
    route_out,
    route_in,
    w_sem,
    in_sem,
    out_sem,
    dense_send,
    pass_send,
    visit_recv,
    route_send,
    route_recv,
    tally_send,
    tally_recv,
    near_send,
    near_recv,
    lodge_send,
    lodge_recv,
    far_send,
    far_recv,
    near_rsend,
    near_rrecv,
    far_rsend,
    far_rrecv,
    back_send,
    back_recv,
):
    me = lax.axis_index("expert")
    group = lax.axis_index("groups")
    lanes = n // 4
    half = 2 * lanes
    mirror = 3 * lanes
    rows, width = x_hbm.shape
    span = half * slot
    cross = lanes // 2
    block = lanes * slot
    part = width // chunks
    hid = w1.shape[1]
    padded = counts.shape[2]
    copies, task_width = n // (2 * SHARED), n // (2 * TASKS)
    plane = me // lanes
    inner = plane // 2 + plane % 2 == 1
    outer = plane // 2 + plane % 2 != 1

    barrier = pltpu.get_barrier_semaphore()

    def peer(d):
        return (group, flip(me, d, n))

    with jax.named_scope('signals'):
        each(
            1,
            n,
            lambda d: pl.semaphore_signal(
                barrier, inc=1, device_id=peer(d), device_id_type=MESH
            ),
        )

    inputs = [
        pltpu.make_async_copy(src, dst, in_sem.at[i])
        for i, (src, dst) in enumerate(
            (
                (label_hbm, label_ref),
                (sel_hbm, sel_ref),
                (mix_hbm, mix_ref),
                (x_hbm, x_ref),
                (room_hbm, room_ref),
            )
        )
    ]
    for load in inputs:
        load.start()
    load1 = pltpu.make_async_copy(w1_hbm.at[0], w1, w_sem.at[0])
    load2 = pltpu.make_async_copy(w2_hbm.at[0], w2, w_sem.at[1])

    def remote(src, dst, send, recv, d):
        return pltpu.make_async_remote_copy(
            src_ref=src,
            dst_ref=dst,
            send_sem=send,
            recv_sem=recv,
            device_id=peer(d),
            device_id_type=MESH,
        )

    def at(first, d, k=None):
        start = first + d * slot
        if not isinstance(start, int):
            start = pl.multiple_of(start, slot)
        if k is None:
            return (pl.ds(start, slot), slice(None))
        return (pl.ds(start, slot), pl.ds(k * part, part))

    def columns(k):
        return (slice(None), pl.ds(k * part, part))

    def tally(d):
        return remote(counts.at[0], counts.at[d], tally_send, tally_recv, d)

    def route(i, j, d):
        return remote(
            route_out.at[i], route_in.at[j], route_send.at[i], route_recv.at[j], d
        )

    def dense(j, d, k):
        return remote(
            x_ref.at[columns(k)],
            visits.at[(j,) + columns(k)],
            dense_send,
            visit_recv.at[j, k],
            d,
        )

    def pass_on(k):
        return remote(
            visits.at[(2,) + columns(k)],
            visits.at[(1,) + columns(k)],
            pass_send,
            visit_recv.at[1, k],
            mirror,
        )

    def near(side, l, part=0):
        d = side * lanes + l
        return remote(
            outgoing.at[at(0, d)],
            inbox.at[at(0, d)],
            near_send,
            near_recv.at[side + part],
            d,
        )

    def lodge(l, k):
        return remote(
            relayed.at[(2,) + at(0, l, k)],
            inbox.at[at(block, l, k)],
            lodge_send,
            lodge_recv,
            l,
        )

    def far(g, side, l, k):
        d = side * lanes + l
        return remote(
            relayed.at[(g,) + at(0, d, k)],
            inbox.at[at((2 + g) * block, l, k)],
            far_send.at[g],
            far_recv.at[g],
            d,
        )

    def near_answer(d):
        return remote(
            results.at[at(0, d)], returned.at[at(0, d)], near_rsend, near_rrecv, d
        )

    def far_answer(g, side, l, k):
        d = side * lanes + l
        return remote(
            results.at[at((2 + g) * block, l, k)],
            relay_in.at[(g,) + at(0, d, k)],
            far_rsend.at[g],
            far_rrecv.at[g, k],
            d,
        )

    def back(g, k):
        return remote(
            home_out.at[(g,) + columns(k)],
            home_in.at[columns(k)],
            back_send,
            back_recv.at[k],
            mirror if g == 0 else half,
        )

    def put(k):
        return pltpu.make_async_copy(
            out_ref.at[columns(k)], out_hbm.at[columns(k)], out_sem.at[k]
        )

    def bulk(sem, count, k=None):
        area = inbox.at[pl.ds(0, count * slot)]
        if k is not None:
            area = inbox.at[(pl.ds(0, count * slot), pl.ds(k * part, part))]
        return pltpu.make_async_copy(area, area, sem)

    def enter():
        with jax.named_scope('barrier'):
            pl.semaphore_wait(barrier, n - 1)

    def send_rows():
        route(1, 2, lanes).start()
        route(0, 1, half).start()
        for k in range(chunks):
            dense(2, lanes, k).start()

    with jax.named_scope('wait_small'):
        for load in inputs[:3]:
            load.wait()
    lane = lax.broadcasted_iota(jnp.int32, (1, rows), 1)
    task_id = SHARED * copies + label_ref[...] * task_width + sel_ref[0:1, :] - SHARED
    shared_id = sel_ref[1:2, :] * copies + lane % copies
    expert = lax.broadcasted_iota(jnp.int32, (padded, rows), 0)
    task_hot = (expert == task_id).astype(jnp.float32)
    shared_hot = (expert == shared_id).astype(jnp.float32)
    hot = (task_hot + shared_hot).astype(jnp.bfloat16)
    earlier = (
        lax.broadcasted_iota(jnp.int32, (rows, rows), 0)
        < lax.broadcasted_iota(jnp.int32, (rows, rows), 1)
    ).astype(jnp.float32)
    before = jnp.dot(
        hot, earlier.astype(jnp.bfloat16), preferred_element_type=jnp.float32
    )
    task_rank = jnp.sum(before * task_hot, axis=0, keepdims=True)
    shared_rank = jnp.sum(before * shared_hot, axis=0, keepdims=True)
    counts[0] = lax.dot_general(
        jnp.ones((8, rows), jnp.bfloat16),
        hot,
        (((1,), (1,)), ((), ())),
        preferred_element_type=jnp.float32,
    )[:1]

    task_near = (task_id ^ me) < half
    near_id = jnp.where(task_near, task_id, shared_id)
    far_id = jnp.where(task_near, shared_id, task_id)
    near_rank = jnp.where(task_near, task_rank, shared_rank).astype(jnp.int32)
    far_rank = jnp.where(task_near, shared_rank, task_rank).astype(jnp.int32)
    near_slot = (near_id ^ me) * slot + near_rank
    relay = flip(me, half, n) * (1 - inner.astype(jnp.int32)) + flip(
        me, mirror, n
    ) * inner.astype(jnp.int32)
    route_out[0] = (far_id ^ relay) * slot + far_rank
    route_out[1] = (near_id ^ flip(me, lanes, n)) * slot + near_rank

    @pl.when(plane == 3)
    def _():
        with jax.named_scope('wait_x'):
            inputs[3].wait()
        enter()
        send_rows()
        load1.start()
        load2.start()

    @pl.when(plane != 3)
    def _():
        inputs[3].wait()
        load1.start()
        load2.start()

    def choice(slots, count):
        slot_row = lax.broadcasted_iota(jnp.int32, (count, rows), 0)
        return (slot_row == slots).astype(jnp.float32).astype(jnp.bfloat16)

    def pack(chosen, block_rows):
        return jnp.dot(chosen, block_rows, preferred_element_type=jnp.float32).astype(
            jnp.bfloat16
        )

    with jax.named_scope('near_pack'):
        near_pack = pack(choice(near_slot, span), x_ref[...])
        outgoing[...] = near_pack
        inbox[pl.ds(0, slot)] = near_pack[:slot]

    tile = hid
    out_tile = min(512, width)

    def expand(first, count):
        @pl.loop(0, hid // tile)
        def _(t):
            cols = pl.ds(pl.multiple_of(t * tile, tile), tile)
            h = jnp.dot(
                inbox[pl.ds(first, count)],
                w1[:, cols],
                preferred_element_type=jnp.float32,
            )
            hidden[:count, cols] = jax.nn.gelu(h).astype(jnp.bfloat16)

    def shrink(first, count, cols):
        y = jnp.dot(
            hidden[:count], w2[:, cols], preferred_element_type=jnp.float32
        )
        results[pl.ds(first, count), cols] = y.astype(jnp.bfloat16)

    def near_work(first, count):
        expand(first, count)

        @pl.loop(0, width // out_tile)
        def _(t):
            cols = pl.ds(pl.multiple_of(t * out_tile, out_tile), out_tile)
            shrink(first, count, cols)

        if first == 0:
            returned[pl.ds(0, slot)] = results[pl.ds(0, slot)]

    def far_work(g, send):
        with jax.named_scope(f'far_expand{g}'):
            expand((2 + g) * block, block)
        with jax.named_scope(f'far_shrink{g}'):
            pair = min(4, chunks)
            for j in range(chunks // pair):
                shrink((2 + g) * block, block, pl.ds(j * pair * part, pair * part))
                for k in range(j * pair, (j + 1) * pair):
                    send(k)

    def column(row):
        return jnp.broadcast_to(row, (128, row.shape[1])).T[:, :1]

    def reader(slots):
        slot_lane = lax.broadcasted_iota(jnp.int32, (rows, span), 1).astype(jnp.float32)
        slots = column(slots.astype(jnp.float32))
        return (slot_lane == slots).astype(jnp.float32).astype(jnp.bfloat16)

    def weigh():
        pltpu.make_async_copy(counts.at[pl.ds(1, n - 1)], counts.at[pl.ds(1, n - 1)], tally_recv).wait()
        inputs[4].wait()
        offset = jnp.zeros((1, padded), jnp.float32)
        for d in range(1, n):
            offset = offset + counts[d] * jnp.where(flip(me, d, n) < me, 1.0, 0.0)
        offset = column(offset)
        arrival_task = task_rank + jnp.sum(task_hot * offset, axis=0, keepdims=True)
        arrival_shared = shared_rank + jnp.sum(
            shared_hot * offset, axis=0, keepdims=True
        )
        room_task = jnp.zeros((1, rows), jnp.int32)
        room_shared = jnp.zeros((1, rows), jnp.int32)
        for e in range(n):
            size = room_ref[e]
            if e < half:
                room_shared = jnp.where(shared_id == e, size, room_shared)
            else:
                room_task = jnp.where(task_id == e, size, room_task)
        keep_task = (arrival_task < room_task.astype(jnp.float32)).astype(jnp.float32)
        keep_shared = (arrival_shared < room_shared.astype(jnp.float32)).astype(
            jnp.float32
        )
        mix = mix_ref[...].astype(jnp.float32)
        total = mix[0:1] + mix[1:2]
        task_weight = mix[0:1] / total * keep_task
        shared_weight = mix[1:2] / total * keep_shared
        weights[0] = column(jnp.where(task_near, task_weight, shared_weight))
        weights[1] = column(jnp.where(task_near, shared_weight, task_weight))

    @pl.when(plane != 3)
    def _():
        enter()

    @pl.when(outer)
    def _():
        @pl.when(plane == 0)
        def _():
            send_rows()

        each(1, lanes, lambda l: near(0, l).start())
        each(1, n, lambda d: tally(d).start())

        def own():
            with jax.named_scope('o_wait_own'):
                bulk(near_recv.at[0], lanes - 1).wait()
            with jax.named_scope('o_work0'):
                near_work(0, block)

        def reply():
            each(1, lanes, lambda d: near_answer(d).start())

        def other(lo, hi, part):
            with jax.named_scope(f'o_wait_other{part}'):
                bulk(near_recv.at[1 + part], hi - lo).wait()
            with jax.named_scope(f'o_work1{part}'):
                near_work(block + lo * slot, (hi - lo) * slot)
            each(lanes + lo, lanes + hi, lambda d: near_answer(d).start())

        def far_step(g):
            def send(k):
                each(0, lanes, lambda l: far_answer(g, 1, l, k).start())

            with jax.named_scope(f'o_far_wait{g}'):
                bulk(far_recv.at[g], lanes).wait()
            far_work(g, send)

        def weigh_step():
            with jax.named_scope('o_weigh'):
                weigh()

        steps = {"own": own, "reply": reply, "other0": functools.partial(other, 0, cross, 0), "other1": functools.partial(other, cross, lanes, 1), "weigh": weigh_step}
        for g in range(2):
            steps[f"far{g}"] = functools.partial(far_step, g)
        load1.wait()
        load2.wait()
        for step in OUTER:
            steps[step]()

    @pl.when(inner)
    def _():
        route(0, 0, mirror).start()
        for k in range(chunks):
            dense(0, mirror, k).start()
        each(0, cross, lambda l: near(1, l).start())
        each(1, lanes, lambda l: near(0, l).start())
        each(1, n, lambda d: tally(d).start())

        def host(g, chosen, k):
            packed = pack(chosen, visits[(g,) + columns(k)])
            relayed[(g, slice(None), pl.ds(k * part, part))] = packed
            inbox[at((2 + g) * block, 0, k)] = packed[:slot]
            each(1, lanes, lambda l: far(g, 0, l, k).start())
            each(0, lanes, lambda l: far(g, 1, l, k).start())

        def guest0():
            route(1, 2, lanes).wait_recv()
            route(0, 0, mirror).wait_recv()
            lodge_choice = choice(route_in[2], block)
            guest_choice = choice(route_in[0], span)
            for k in range(chunks):
                with jax.named_scope(f'i_waitG{k}'):
                    dense(2, lanes, k).wait_recv()
                pass_on(k).start()
                with jax.named_scope(f'i_waitg0_{k}'):
                    dense(0, mirror, k).wait_recv()
                with jax.named_scope(f'i_host0_{k}'):
                    host(0, guest_choice, k)
                packed = pack(lodge_choice, visits[(2,) + columns(k)])
                relayed[(2, pl.ds(0, block), pl.ds(k * part, part))] = packed
                inbox[at(block, 0, k)] = packed[:slot]
                each(1, lanes, lambda l: lodge(l, k).start())
            load1.wait()
            load2.wait()

        def own():
            with jax.named_scope('i_wait_own'):
                bulk(near_recv.at[0], lanes - 1).wait()
            with jax.named_scope('i_work0'):
                near_work(0, block)

        def reply():
            each(1, lanes, lambda d: near_answer(d).start())

        def guest1():
            route(0, 1, half).wait_recv()
            guest_choice = choice(route_in[1], span)
            for k in range(chunks):
                with jax.named_scope(f'i_waitg1_{k}'):
                    pass_on(k).wait_recv()
                with jax.named_scope(f'i_host1_{k}'):
                    host(1, guest_choice, k)
            each(cross, lanes, lambda l: near(1, l, 1).start())

        def lodged():
            with jax.named_scope('i_waitlodge'):
                bulk(lodge_recv, lanes - 1).wait()
            with jax.named_scope('i_work1'):
                near_work(block, block)
            each(lanes, half, lambda d: near_answer(d).start())

        def take_back(g, lo, hi):
            guest_reader = reader(route_in[g])
            for k in range(lo, hi):
                with jax.named_scope(f'i_waitans{g}_{k}'):
                    bulk(far_rrecv.at[g, k], half - 1, k).wait()
                home_out[(g,) + columns(k)] = pack(
                    guest_reader, relay_in[(g, slice(None), pl.ds(k * part, part))]
                )
                back(g, k).start()

        def far_step(g):
            def send(k):
                each(1, lanes, lambda l: far_answer(g, 0, l, k).start())
                relay_in[(g,) + at(0, 0, k)] = results[at((2 + g) * block, 0, k)]

            with jax.named_scope(f'i_far_wait{g}'):
                bulk(far_recv.at[g], lanes - 1).wait()
            far_work(g, send)

        def weigh_step():
            with jax.named_scope('i_weigh'):
                weigh()

        steps = {"own": own, "reply": reply, "guest0": guest0, "guest1": guest1, "lodge": lodged, "weigh": weigh_step}
        for g in range(2):
            steps[f"far{g}"] = functools.partial(far_step, g)
            steps[f"back{g}"] = functools.partial(take_back, g, 0, chunks)
            steps[f"back{g}a"] = functools.partial(take_back, g, 0, chunks // 2)
            steps[f"back{g}b"] = functools.partial(take_back, g, chunks // 2, chunks)
        for step in INNER:
            steps[step]()

    near_reader = reader(near_slot)
    with jax.named_scope('wait_near_ans'):
        bulk(near_rrecv, half - 1).wait()
    partial[...] = (
        jnp.dot(near_reader, returned[...], preferred_element_type=jnp.float32)
        * weights[0]
    )
    far_weight = weights[1]
    for k in range(chunks):
        with jax.named_scope(f'wait_back{k}'):
            back(0, k).wait_recv()
        out_ref[columns(k)] = (
            partial[columns(k)] + home_in[columns(k)].astype(jnp.float32) * far_weight
        ).astype(jnp.bfloat16)
        put(k).start()

    with jax.named_scope('drain'):
        pltpu.make_async_copy(
            counts.at[pl.ds(1, n - 1)], counts.at[pl.ds(1, n - 1)], tally_send
        ).wait()
        bulk(near_rsend, half - 1).wait()
        route(0, 0, mirror).wait_send()
        pltpu.make_async_copy(x_ref, home_in, dense_send).wait()

        @pl.when(outer)
        def _():
            route(1, 2, lanes).wait_send()
            bulk(near_send, lanes - 1).wait()
            for g in range(2):
                bulk(far_rsend.at[g], lanes).wait()

        @pl.when(inner)
        def _():
            bulk(near_send, half - 1).wait()
            pltpu.make_async_copy(x_ref, home_in, pass_send).wait()
            bulk(lodge_send, lanes - 1).wait()
            for g in range(2):
                bulk(far_send.at[g], half - 1).wait()
                bulk(far_rsend.at[g], lanes - 1).wait()
            pltpu.make_async_copy(home_out, home_out, back_send).wait()

        for k in range(chunks):
            put(k).wait()


def solution(mesh):
    n = mesh.shape["expert"]

    def shards(x, label, sel, mix, room, first, second):
        rows, width = x.shape
        hid = first.shape[2]
        slot = -(-(4 * rows // n) // 16) * 16
        lanes, half = n // 4, n // 2
        chunks = CHUNKS if lanes <= 8 else 1
        padded = -(-n // 128) * 128
        bf16, f32, i32 = jnp.bfloat16, jnp.float32, jnp.int32
        anywhere = pl.BlockSpec(memory_space=pltpu.HBM)
        dma = pltpu.SemaphoreType.DMA
        return pl.pallas_call(
            functools.partial(kernel, n, slot, chunks),
            out_shape=jax.ShapeDtypeStruct((rows, width), bf16),
            in_specs=[anywhere] * 7,
            out_specs=anywhere,
            scratch_shapes=[
                pltpu.SMEM((n,), i32),
                pltpu.VMEM((1, rows), i32),
                pltpu.VMEM((2, rows), i32),
                pltpu.VMEM((2, rows), i32),
                pltpu.VMEM((rows, width), bf16),
                pltpu.VMEM((rows, width), bf16),
                pltpu.VMEM(first.shape[1:], bf16),
                pltpu.VMEM(second.shape[1:], bf16),
                pltpu.VMEM((3, rows, width), bf16),
                pltpu.VMEM((half * slot, width), bf16),
                pltpu.VMEM((3, half * slot, width), bf16),
                pltpu.VMEM((n * slot, width), bf16),
                pltpu.VMEM((lanes * slot, hid), bf16),
                pltpu.VMEM((n * slot, width), bf16),
                pltpu.VMEM((half * slot, width), bf16),
                pltpu.VMEM((2, half * slot, width), bf16),
                pltpu.VMEM((2, rows, width), bf16),
                pltpu.VMEM((rows, width), bf16),
                pltpu.VMEM((rows, width), f32),
                pltpu.VMEM((2, rows, 1), f32),
                pltpu.VMEM((n, 1, padded), f32),
                pltpu.VMEM((2, 1, rows), i32),
                pltpu.VMEM((3, 1, rows), i32),
                dma((2,)),
                dma((5,)),
                dma((chunks,)),
                dma(()),
                dma(()),
                dma((3, chunks)),
                dma((2,)),
                dma((3,)),
                dma(()),
                dma(()),
                dma(()),
                dma((3,)),
                dma(()),
                dma(()),
                dma((2,)),
                dma((2,)),
                dma(()),
                dma(()),
                dma((2,)),
                dma((2, chunks)),
                dma(()),
                dma((chunks,)),
            ],
            compiler_params=pltpu.CompilerParams(
                collective_id=0, has_side_effects=True, vmem_limit_bytes=LIMIT
            ),
        )(room, label.reshape(1, rows), sel.T, mix.T, x, first, second)

    in_specs = (
        P(("groups", "expert"), None),
        P(("groups", "expert")),
        P(("groups", "expert"), None),
        P(("groups", "expert"), None),
        P(),
        P("expert", None, None),
        P("expert", None, None),
    )
    return jax.shard_map(
        shards,
        mesh=mesh,
        in_specs=in_specs,
        out_specs=P(("groups", "expert"), None),
        check_vma=False,
    )
```
